256 devices in a mesh: dp: 64 (over z_lo, x, y), mp: 4 (over z_hi, core).
Axes of the slice: x: 4, y: 4, z: 8 (z_hi: 2, z_lo: 4; z = z_hi * 4 + z_lo), core: 2. Of those that a mesh axis runs over, the one named last changes fastest.
Arguments:
- features: bfloat16 [16384, 7168], P('dp', 'mp'), may hold values from -6 to 6
- projection: bfloat16 [7168, 256], replicated, may hold values from -0.375 to 0.375
- out_grad: bfloat16 [16384, 20480], P('dp', 'mp'), may hold values from -64 to 64
- momentum: float32 [7168, 20480], P('dp', 'mp'), may hold values from -2 to 2
Outputs:
- new_momentum: float32 [7168, 20480], P('dp', 'mp')
The draws below stay inside these ranges and needn't reach their ends.
All inputs are finite; a program needn't handle non-finite values.
Results may differ from the reference program's by a relative error of at most 0.0011.
Values may be sent and summed in bfloat16 or wider, within the bound.
A program may use at most 64 MiB of HBM per device.

```python
import math
import jax
import jax.numpy as jnp
from jax import lax

D = 7168
FF = 20480
R = 256
TOKENS = 16384


def draw_out_grad(key, part):
    keys = jax.random.split(jax.random.fold_in(key, 11), 3)
    normal_part = jax.random.truncated_normal(keys[0], -4.0, 4.0, (TOKENS, FF), jnp.float32)
    row_scale = jnp.exp(jax.random.uniform(keys[1], (TOKENS, 1), jnp.float32, math.log(0.3), math.log(3.0)))
    position = jnp.arange(FF, dtype=jnp.float32) / FF
    col_scale = jnp.exp(jax.random.uniform(keys[2], (1, FF), jnp.float32, math.log(0.4), math.log(4.0)))
    col_scale = col_scale * jnp.exp(math.log(3.0) * (position - 0.5))[None, :]
    values = normal_part
    return jnp.clip(values * row_scale * col_scale, -64.0, 64.0).astype(jnp.bfloat16)


def steps_of(rng, extent, shards, low, high):
    def one(axis_at, shards_of):
        heights = jax.random.uniform(jax.random.fold_in(jax.random.fold_in(rng, 6), axis_at), (shards_of,), jnp.float32, low / len(shards), high / len(shards))
        return jnp.repeat(jnp.exp(heights), extent[axis_at] // shards_of).reshape((-1,) + (1,) * (len(extent) - axis_at - 1))

    loudness = one(*shards[0])
    for cut in shards[1:]:
        loudness = loudness * one(*cut)
    return loudness


def bell_draw(own_key, dims, width, limit, pieces=(), held_as=jnp.bfloat16):
    array = jax.random.normal(own_key, dims, jnp.float32) * width
    if len(pieces) > 0:
        array = steps_of(own_key, dims, pieces, -0.22, 0.18) * array
    return jnp.clip(array, min=-limit, max=limit).astype(held_as)


def setup_inputs(seed: int = 0) -> dict:
    streams_of = jax.random.split(jax.random.key(seed), 5)
    features = bell_draw(streams_of[0], (TOKENS, D), 1.0, 6.0, ((0, 64), (1, 4)))
    projection = bell_draw(streams_of[1], (D, R), R ** -0.5, 0.375)
    out_grad = draw_out_grad(jax.random.fold_in(streams_of[4], 71), 0)
    momentum = bell_draw(streams_of[3], (D, FF), 0.3, 2.0, ((0, 64), (1, 4)), jnp.float32)
    return dict(features=features, projection=projection, out_grad=out_grad, momentum=momentum)


def reference(features, projection, out_grad, momentum):
    mixed_rows = jnp.dot(features, projection, preferred_element_type=jnp.float32).astype(jnp.bfloat16)
    full_panel = jnp.dot(out_grad.T, mixed_rows, preferred_element_type=jnp.float32)
    square_sum = jnp.sum(full_panel * full_panel)
    factor = jnp.float32(math.sqrt(R * FF)) / jnp.sqrt(square_sum + 1e-06)
    decoded = jnp.dot(projection.astype(jnp.float32), full_panel.T, precision=lax.Precision.HIGHEST, preferred_element_type=jnp.float32)
    return 0.9 * momentum + 0.1 * factor * decoded
```

```python
import math

import jax
import jax.numpy as jnp
from jax import lax
from jax.experimental import pallas as pl
from jax.experimental.pallas import tpu as pltpu
from jax.sharding import Mesh
from jax.sharding import PartitionSpec as P

MESH = pl.DeviceIdType.MESH
D = 7168
FF = 20480
R = 256
TOK = 256
KF = 1792
ROWS = 112
CH = 640
HALF = 2560
WIRE = jnp.float32

MP = ("zh", "c")
DP = ("zl", "x", "y")
PEERS = ("x", "y", "zl")


def dot(a, b):
    return jnp.dot(a, b, preferred_element_type=jnp.float32)


def tile_squares(v):
    rows, cols = v.shape
    total = jnp.zeros((8, 128), jnp.float32)
    for i in range(rows // 8):
        for j in range(cols // 128):
            part = v[8 * i : 8 * i + 8, 128 * j : 128 * j + 128]
            total = total + part * part
    return total


def kernel(
    f_hbm, p_hbm, g_hbm, m_hbm, out_ref,
    f_v, p_v, g_v, mom_v, pd_v,
    mpart, mrecv, msum, mixed, mixed_own,
    panel, crecv, quart, drecv, full,
    dec_s, dec_r, sq,
    load_sem, g_ss, g_rs, m_ss, m_rs, x_ss, x_rs, fw_ss, fw_rs,
    c_ss, c_rs, d_ss, d_rs, e_ss, e_rs, h_ss, h_rs, o_ss, o_rs, q_ss, q_rs,
):
    pos = {a: lax.axis_index(a) for a in ("zl", "x", "y", "zh", "c")}
    sent = []

    def aligned(i, n):
        return pl.multiple_of(i * n, n)

    def send(src, dst, ss, rs, axis, where):
        copy = pltpu.make_async_remote_copy(
            src_ref=src, dst_ref=dst, send_sem=ss, recv_sem=rs,
            device_id={axis: where}, device_id_type=MESH,
        )
        copy.start()
        sent.append(copy)
        return copy

    def ahead(axis, d):
        return lax.rem(pos[axis] + d, 4)

    other = {"zh": 1 - pos["zh"], "c": 1 - pos["c"]}

    loads = {}

    def load(name, src, dst):
        copy = pltpu.make_async_copy(src, dst, load_sem.at[len(loads)])
        copy.start()
        loads[name] = copy

    mp = pos["zh"] * 2 + pos["c"]
    load("f", f_hbm, f_v)
    load("p", p_hbm.at[pl.ds(aligned(mp, KF), KF), :], p_v)
    sets = ("x", "y")
    for s, axis in enumerate(sets):
        load(("g", s), g_hbm.at[:, pl.ds(pl.multiple_of(s * HALF + pos[axis] * CH, 128), CH)], g_v.at[s, 0])
    base = pos["zl"] * 16
    for d in range(4):
        row = base + ahead("x", d) * 4 + pos["y"]
        load(("p", 0, d), p_hbm.at[pl.ds(aligned(row, ROWS), ROWS), :], pd_v.at[0, d])
        row = base + pos["x"] * 4 + ahead("y", d)
        load(("p", 1, d), p_hbm.at[pl.ds(aligned(row, ROWS), ROWS), :], pd_v.at[1, d])
    load("m", m_hbm, mom_v)

    barrier = pltpu.get_barrier_semaphore()
    for axis in PEERS:
        for d in (1, 2, 3):
            pl.semaphore_signal(barrier, inc=1, device_id={axis: ahead(axis, d)}, device_id_type=MESH)
    for axis in ("zh", "c"):
        pl.semaphore_signal(barrier, inc=1, device_id={axis: other[axis]}, device_id_type=MESH)

    loads["f"].wait()
    loads["p"].wait()
    mpart[...] = dot(f_v[...], p_v[...])

    pl.semaphore_wait(barrier, 11)

    mine = pl.ds(aligned(pos["c"], 128), 128)
    theirs = pl.ds(aligned(other["c"], 128), 128)
    m1 = send(mpart.at[theirs, :], mrecv.at[0], m_ss.at[0], m_rs.at[0], "c", other["c"])

    got = {}
    for d in (2, 1, 3):
        for s, axis in enumerate(sets):
            peer = ahead(axis, d)
            got[s, 4 - d] = send(
                g_hbm.at[:, pl.ds(pl.multiple_of(s * HALF + peer * CH, 128), CH)],
                g_v.at[s, 4 - d], g_ss.at[s, d], g_rs.at[s, 4 - d], axis, peer,
            )

    m1.wait_recv()
    msum[...] = mpart[mine, :] + mrecv[0]
    m2 = send(msum, mrecv.at[1], m_ss.at[1], m_rs.at[1], "zh", other["zh"])
    m2.wait_recv()
    mixed_own[:, mine] = (msum[...] + mrecv[1]).T.astype(jnp.bfloat16)
    own = send(mixed_own.at[:, mine], mixed_own.at[:, mine], m_ss.at[2], m_rs.at[2], "c", other["c"])
    direct = {}
    for d in (2, 1, 3):
        for s, axis in enumerate(sets):
            direct[s, 4 - d] = send(
                mixed_own.at[:, mine], mixed.at[s, 4 - d, :, mine],
                x_ss.at[s, d], x_rs.at[s, 4 - d], axis, ahead(axis, d),
            )
    passed = {}
    order = [(s, k) for k in (1, 3, 2) for s in (0, 1)]
    for s, k in order:
        direct[s, k].wait_recv()
        passed[s, k] = send(
            mixed.at[s, k, :, mine], mixed.at[s, k, :, mine],
            fw_ss.at[s, k], fw_rs.at[s, k], "c", other["c"],
        )

    own.wait_recv()
    for s in (0, 1):
        loads["g", s].wait()
        panel[s] = dot(mixed_own[...], g_v[s, 0])
    for s, k in order:
        passed[s, k].wait_recv()
        got[s, k].wait_recv()
        panel[s] += dot(mixed[s, k], g_v[s, k])

    cross = ("y", "x")
    arrived = {}
    for d in (2, 1, 3):
        for s, axis in enumerate(cross):
            peer = ahead(axis, d)
            arrived[s, d] = send(
                panel.at[s, pl.ds(aligned(peer, 64), 64), :], crecv.at[s, d - 1],
                c_ss.at[s, d], c_rs.at[s, d], axis, peer,
            )
    for s, axis in enumerate(cross):
        for d in (1, 2, 3):
            arrived[s, d].wait_recv()
        quart[s] = (panel[s, pl.ds(aligned(pos[axis], 64), 64), :] + crecv[s, 0]) + (crecv[s, 1] + crecv[s, 2])
    arrived = {}
    for d in (3, 2, 1):
        for s in (0, 1):
            peer = ahead("zl", d)
            arrived[s, d] = send(
                quart.at[s, pl.ds(aligned(peer, 16), 16), :], drecv.at[s, d - 1],
                d_ss.at[s, d], d_rs.at[s, d], "zl", peer,
            )
    squares = jnp.zeros((8, 128), jnp.float32)
    pieces = []
    for s, axis in enumerate(cross):
        for d in (1, 2, 3):
            arrived[s, d].wait_recv()
        total = (quart[s, pl.ds(aligned(pos["zl"], 16), 16), :] + drecv[s, 0]) + (drecv[s, 1] + drecv[s, 2])
        piece = pl.ds(pl.multiple_of(pos[axis] * 64 + pos["zl"] * 16, 16), 16)
        full[s, piece, :] = total
        pieces.append(piece)
        squares = squares + tile_squares(total)

    sq[0, 0] = squares

    def spread(level, axis):
        return [send(sq.at[level, 0], sq.at[level, d], q_ss.at[level, d], q_rs.at[level, d], axis, ahead(axis, d)) for d in (1, 2, 3)]

    def collect(level, copies):
        for copy in copies:
            copy.wait_recv()
        sq[level + 1, 0] = (sq[level, 0] + sq[level, 1]) + (sq[level, 2] + sq[level, 3])

    def pair(level, axis):
        return send(sq.at[level, 0], sq.at[level, 1], q_ss.at[level, 1], q_rs.at[level, 1], axis, other[axis])

    arrived = {}
    for d in (3, 2, 1):
        for s in (0, 1):
            arrived[s, d] = send(
                full.at[s, pieces[s], :], full.at[s, pieces[s], :],
                e_ss.at[s, d], e_rs.at[s, d], "zl", ahead("zl", d),
            )
    q = spread(0, "zl")
    for s in (0, 1):
        for d in (1, 2, 3):
            arrived[s, d].wait_recv()
    arrived = {}
    for d in (2, 1, 3):
        for s, axis in enumerate(cross):
            block = pl.ds(aligned(pos[axis], 64), 64)
            arrived[s, d] = send(
                full.at[s, block, :], full.at[s, block, :],
                h_ss.at[s, d], h_rs.at[s, d], axis, ahead(axis, d),
            )
    collect(0, q)
    q = spread(1, "y")
    collect(1, q)
    q = spread(2, "x")
    for s in (0, 1):
        for d in (1, 2, 3):
            arrived[s, d].wait_recv()

    final = {}
    for s, axis in enumerate(sets):
        whole = full[s]
        high = whole.astype(jnp.bfloat16)
        low = (whole - high.astype(jnp.float32)).astype(jnp.bfloat16)
        for d in (2, 1, 3, 0):
            loads["p", s, d].wait()
            rows = dot(pd_v[s, d], high) + dot(pd_v[s, d], low)
            if d == 0:
                dec_r[s, 0] = rows.astype(WIRE)
            else:
                dec_s[s, d - 1] = rows.astype(WIRE)
                final[s, 4 - d] = send(
                    dec_s.at[s, d - 1], dec_r.at[s, 4 - d],
                    o_ss.at[s, d], o_rs.at[s, 4 - d], axis, ahead(axis, d),
                )
    collect(2, q)
    p = pair(3, "c")
    p.wait_recv()
    sq[4, 0] = sq[3, 0] + sq[3, 1]
    p = pair(4, "zh")
    p.wait_recv()
    square_sum = jnp.sum(sq[4, 0] + sq[4, 1], axis=(0, 1), keepdims=True)
    scale = 0.1 * (jnp.float32(math.sqrt(R * FF)) / jnp.sqrt(square_sum + 1e-06))

    loads["m"].wait()
    for k in (0, 1, 3, 2):
        for s, axis in enumerate(sets):
            if k:
                final[s, k].wait_recv()
            cols = pl.ds(pl.multiple_of(s * HALF + ahead(axis, k) * CH, 128), CH)
            out_ref[:, cols] = 0.9 * mom_v[:, cols] + scale * dec_r[s, k].astype(jnp.float32)
    for copy in sent:
        copy.wait_send()


def local(features, projection, out_grad, momentum):
    dma = pltpu.SemaphoreType.DMA
    f32, bf16 = jnp.float32, jnp.bfloat16
    return pl.pallas_call(
        kernel,
        out_shape=jax.ShapeDtypeStruct((ROWS, 2 * HALF), f32),
        in_specs=[pl.BlockSpec(memory_space=pl.ANY)] * 4,
        out_specs=pl.BlockSpec(memory_space=pltpu.VMEM),
        scratch_shapes=[
            pltpu.VMEM((TOK, KF), bf16),
            pltpu.VMEM((KF, R), bf16),
            pltpu.VMEM((2, 4, TOK, CH), bf16),
            pltpu.VMEM((ROWS, 2 * HALF), f32),
            pltpu.VMEM((2, 4, ROWS, R), bf16),
            pltpu.VMEM((TOK, R), f32),
            pltpu.VMEM((2, 128, R), f32),
            pltpu.VMEM((128, R), f32),
            pltpu.VMEM((2, 4, R, TOK), bf16),
            pltpu.VMEM((R, TOK), bf16),
            pltpu.VMEM((2, R, CH), f32),
            pltpu.VMEM((2, 3, 64, CH), f32),
            pltpu.VMEM((2, 64, CH), f32),
            pltpu.VMEM((2, 3, 16, CH), f32),
            pltpu.VMEM((2, R, CH), f32),
            pltpu.VMEM((2, 3, ROWS, CH), WIRE),
            pltpu.VMEM((2, 4, ROWS, CH), WIRE),
            pltpu.VMEM((5, 4, 8, 128), f32),
            dma((16,)),
            dma((2, 4)), dma((2, 4)),
            dma((3,)), dma((3,)),
            dma((2, 4)), dma((2, 4)),
            dma((2, 4)), dma((2, 4)),
            dma((2, 4)), dma((2, 4)),
            dma((2, 4)), dma((2, 4)),
            dma((2, 4)), dma((2, 4)),
            dma((2, 4)), dma((2, 4)),
            dma((2, 4)), dma((2, 4)),
            dma((5, 4)), dma((5, 4)),
        ],
        compiler_params=pltpu.CompilerParams(
            collective_id=0, has_side_effects=True, vmem_limit_bytes=40 * 1024 * 1024,
        ),
        name="flora",
    )(features, projection, out_grad, momentum)


def solution(mesh):
    finer = Mesh(mesh.devices.reshape(4, 4, 4, 2, 2), ("zl", "x", "y", "zh", "c"))
    return jax.shard_map(
        local,
        mesh=finer,
        in_specs=(P(DP, MP), P(), P(DP, MP), P(DP, MP)),
        out_specs=P(DP, MP),
        check_vma=False,
    )
```

```python
import math

import jax
import jax.numpy as jnp
from jax import lax
from jax.experimental import pallas as pl
from jax.experimental.pallas import tpu as pltpu
from jax.sharding import Mesh
from jax.sharding import PartitionSpec as P

MESH = pl.DeviceIdType.MESH
FF = 20480
R = 256
TOK = 256
KF = 1792
ROWS = 112
CH = 640
HALF = 2560
BATCHES = ((0, 384), (384, 256))
C_TYPE = jnp.bfloat16
E_TYPE = jnp.bfloat16
G_TYPE = jnp.bfloat16
EARLY = 1
SEMS = 16 + 6 * len(BATCHES)

MP = ("zh", "c")
DP = ("zl", "x", "y")
RING = ("x", "y")
CROSS = ("y", "x")
BOTH = (0, 1)


def dot(a, b):
    return jnp.dot(a, b, preferred_element_type=jnp.float32)


def tile_squares(v):
    rows, cols = v.shape
    total = jnp.zeros((8, 128), jnp.float32)
    for i in range(rows // 8):
        for j in range(cols // 128):
            part = v[8 * i : 8 * i + 8, 128 * j : 128 * j + 128]
            total = total + part * part
    return total


def kernel(
    f_hbm, p_hbm, g_hbm, m_hbm, out_ref,
    f_v, p_v, g_v, mom_v, pd_v,
    mpart, mrecv, msum, mixed,
    panel, panel_s, crecv, quart, drecv, full,
    dec_s, dec_r, sq,
    load_sem, ss, rs,
):
    pos = {a: lax.axis_index(a) for a in ("zl", "x", "y", "zh", "c")}
    other = {"zh": 1 - pos["zh"], "c": 1 - pos["c"]}
    groups = []
    scope = jax.named_scope

    def aligned(i, n):
        return pl.multiple_of(i * n, n)

    def ahead(axis, d):
        return lax.rem(pos[axis] + d, 4)

    def remote(src, dst, i, where):
        return pltpu.make_async_remote_copy(
            src_ref=src, dst_ref=dst, send_sem=ss.at[i], recv_sem=rs.at[i],
            device_id=where, device_id_type=MESH,
        )

    def send(copies, whole):
        i = len(groups)
        for src, dst, where in copies:
            remote(src, dst, i, where).start()
        group = remote(whole, whole, i, copies[0][2])
        groups.append(group)
        return group

    barrier = pltpu.get_barrier_semaphore()
    z_peers = [{"zl": ahead("zl", d)} for d in (1, 2, 3)]
    z_peers += [{"zl": ahead("zl", d), "zh": other["zh"]} for d in (1, 2, 3)] + [{"zh": other["zh"]}]
    greeted = [{axis: ahead(axis, d)} for axis in RING for d in (1, 2, 3)] + z_peers + [{"c": other["c"]}]
    for where in greeted:
        pl.semaphore_signal(barrier, inc=1, device_id=where, device_id_type=MESH)

    loads = {}

    def load(name, src, dst):
        copy = pltpu.make_async_copy(src, dst, load_sem.at[len(loads)])
        copy.start()
        loads[name] = copy

    mp = pos["zh"] * 2 + pos["c"]
    load("f", f_hbm, f_v)
    load("p", p_hbm.at[pl.ds(aligned(mp, KF), KF), :], p_v)

    def late_loads():
        for s in BOTH:
            first = pl.multiple_of(s * HALF + pos[RING[s]] * CH, 128)
            load(("g", s), g_hbm.at[:, pl.ds(first, CH)], g_v.at[s, pl.ds(0, TOK), :])
        base = pos["zl"] * 16
        for d in range(4):
            row = base + ahead("x", d) * 4 + pos["y"]
            load(("p", 0, d), p_hbm.at[pl.ds(aligned(row, ROWS), ROWS), :], pd_v.at[0, pl.ds(d * ROWS, ROWS), :])
            row = base + pos["x"] * 4 + ahead("y", d)
            load(("p", 1, d), p_hbm.at[pl.ds(aligned(row, ROWS), ROWS), :], pd_v.at[1, pl.ds(d * ROWS, ROWS), :])
        load("m", m_hbm, mom_v)

    mine = pl.ds(aligned(pos["c"], 128), 128)
    theirs = pl.ds(aligned(other["c"], 128), 128)
    ring_order = (2, 1, 3)

    def lanes(b):
        off, width = BATCHES[b]
        return pl.ds(off, width)

    def grad_send(b):
        off, width = BATCHES[b]
        copies = []
        for d in ring_order:
            for s, axis in enumerate(RING):
                peer = ahead(axis, d)
                first = pl.multiple_of(s * HALF + peer * CH + off, 128)
                copies.append((
                    g_hbm.at[:, pl.ds(first, width)], g_v.at[s, pl.ds(d * TOK, TOK), lanes(b)], {axis: peer}
                ))
        return send(copies, g_v.at[:, pl.ds(TOK, 3 * TOK), lanes(b)])

    def sum_send(b):
        cols = lanes(b)
        for s in BOTH:
            panel[s, :, cols] = dot(mixed[s], g_v[s, :, cols])
        source = panel
        if C_TYPE != jnp.float32:
            source = panel_s
            panel_s[:, :, cols] = panel[:, :, cols].astype(C_TYPE)
        copies = []
        for d in ring_order:
            for s, axis in enumerate(CROSS):
                peer = ahead(axis, d)
                copies.append((
                    source.at[s, pl.ds(aligned(peer, 64), 64), cols], crecv.at[s, d - 1, :, cols], {axis: peer}
                ))
        return send(copies, crecv.at[:, :, :, cols])

    half, odd = lax.div(pos["zl"], 2), lax.rem(pos["zl"], 2)
    z_to = (3 - 3 * half, 2 - half, pos["zl"] + 1 - 2 * odd)

    def reduce_send(b, group):
        cols = lanes(b)
        with scope(f"C{b}"):
            group.wait_recv()
        for s, axis in enumerate(CROSS):
            total = panel[s, pl.ds(aligned(pos[axis], 64), 64), cols]
            for d in (1, 2, 3):
                total = total + crecv[s, d - 1, :, cols].astype(jnp.float32)
            quart[s, :, cols] = total
        copies = []
        for j, to in enumerate(z_to):
            for s in BOTH:
                slot = odd if j < 2 else 2
                copies.append((quart.at[s, pl.ds(aligned(to, 16), 16), cols], drecv.at[s, slot, :, cols], {"zl": to}))
        return send(copies, drecv.at[:, :, :, cols])

    squares = []

    def gather_send(b, group):
        cols = lanes(b)
        with scope(f"D{b}"):
            group.wait_recv()
        copies = []
        for s in BOTH:
            total = quart[s, pl.ds(aligned(pos["zl"], 16), 16), cols]
            total = (total + drecv[s, 2, :, cols]) + (drecv[s, 0, :, cols] + drecv[s, 1, :, cols])
            place = pl.ds(pl.multiple_of(pos[CROSS[s]] * 64 + pos["zl"] * 16, 16), 16)
            full[s, place, cols] = total.astype(E_TYPE)
            squares.append(tile_squares(total))
            piece = full.at[s, place, cols]
            copies += [(j, s, piece, piece, {"zl": to}) for j, to in enumerate(z_to)]
        copies = [c[2:] for c in sorted(copies, key=lambda c: c[:2])]
        return send(copies, full.at[:, pl.ds(0, 48), cols])

    def cross_send(b, group):
        cols = lanes(b)
        with scope(f"E{b}"):
            group.wait_recv()
        copies = []
        for d in ring_order:
            for s, axis in enumerate(CROSS):
                block = full.at[s, pl.ds(aligned(pos[axis], 64), 64), cols]
                copies.append((block, block, {axis: ahead(axis, d)}))
        return send(copies, full.at[:, pl.ds(0, 192), cols])

    def decode_send(b, group):
        cols = lanes(b)
        with scope(f"F{b}"):
            group.wait_recv()
        if b == 0:
            for s in BOTH:
                for d in range(4):
                    loads["p", s, d].wait()
        for s in BOTH:
            whole = full[s, :, cols]
            if E_TYPE == jnp.float32:
                high = whole.astype(jnp.bfloat16)
                low = (whole - high.astype(jnp.float32)).astype(jnp.bfloat16)
                rows = dot(pd_v[s], high) + dot(pd_v[s], low)
            else:
                rows = dot(pd_v[s], whole)
            panel[s, pl.ds(0, ROWS), cols] = rows[:ROWS]
            for d in (1, 2, 3):
                dec_s[s, d - 1, :, cols] = rows[d * ROWS : (d + 1) * ROWS].astype(G_TYPE)
        copies = []
        for d in ring_order:
            for s, axis in enumerate(RING):
                copies.append((dec_s.at[s, d - 1, :, cols], dec_r.at[s, d - 1, :, cols], {axis: ahead(axis, d)}))
        return send(copies, dec_r.at[:, :, :, cols])

    def spread(level, peers):
        n = len(peers)
        copies = [(sq.at[level, 0], sq.at[level, 1 + k], where) for k, where in enumerate(peers)]
        return send(copies, sq.at[level, pl.ds(1, n)])

    def collect(level, group, n):
        with scope(f"sq{level}"):
            group.wait_recv()
        total = sq[level, 0]
        for k in range(n):
            total = total + sq[level, 1 + k]
        sq[level + 1, 0] = total

    every = range(len(BATCHES))
    with scope("barrier"):
        pl.semaphore_wait(barrier, len(greeted))
    grads = [grad_send(b) for b in every[:EARLY]]
    with scope("mpart"):
        loads["f"].wait()
        loads["p"].wait()
        mpart[...] = dot(f_v[...], p_v[...])
    m1 = send([(mpart.at[theirs, :], mrecv.at[0], {"c": other["c"]})], mrecv.at[0])
    late_loads()
    with scope("m1"):
        m1.wait_recv()
    msum[...] = mpart[mine, :] + mrecv[0]
    m2 = send([(msum, mrecv.at[1], {"zh": other["zh"]})], msum)
    with scope("m2"):
        m2.wait_recv()
    own = (msum[...] + mrecv[1]).T.astype(jnp.bfloat16)
    for s in BOTH:
        mixed[s, :, mine] = own

    def lane_of(d, c):
        return pl.ds(pl.multiple_of(d * TOK + c * 128, 128), 128)

    core = {"c": other["c"]}
    own = mixed.at[0, :, mine]
    direct = {}
    for d in ring_order:
        for s, axis in enumerate(RING):
            there = mixed.at[s, :, lane_of(d, pos["c"])]
            direct[s, d] = send([(own, there, {axis: ahead(axis, d)})], own)
    passed = [send([(mixed.at[s, :, mine], mixed.at[s, :, mine], core) for s in BOTH], mixed.at[:, :, pl.ds(0, 128)])]
    grads += [grad_send(b) for b in every[EARLY:]]
    for d in (1, 3, 2):
        copies = []
        for s in BOTH:
            with scope(f"direct{s}{d}"):
                direct[s, d].wait_recv()
            here = mixed.at[s, :, lane_of(d, pos["c"])]
            copies.append((here, here, core))
        passed.append(send(copies, mixed.at[:, :, pl.ds(d * TOK, 128)]))
    with scope("passed"):
        for group in passed:
            group.wait_recv()
        for s in BOTH:
            loads["g", s].wait()
    moving = []
    for b in every:
        with scope(f"got{b}"):
            grads[b].wait_recv()
        moving.append(sum_send(b))
    moving = [reduce_send(b, moving[b]) for b in every]
    moving = [gather_send(b, moving[b]) for b in every]
    total = squares[0]
    for one in squares[1:]:
        total = total + one
    sq[0, 0] = total
    q = spread(0, [{"y": ahead("y", d)} for d in (1, 2, 3)])
    moving = [cross_send(b, moving[b]) for b in every]
    collect(0, q, 3)
    q = spread(1, [{"x": ahead("x", d)} for d in (1, 2, 3)])
    final = [decode_send(b, moving[b]) for b in every[:-1]]
    collect(1, q, 3)
    q = spread(2, z_peers)
    final.append(decode_send(every[-1], moving[-1]))
    collect(2, q, 7)
    q = spread(3, [core])
    collect(3, q, 1)
    square_sum = jnp.sum(sq[4, 0], axis=(0, 1), keepdims=True)
    scale = 0.1 * (jnp.float32(math.sqrt(R * FF)) / jnp.sqrt(square_sum + 1e-06))

    loads["m"].wait()

    def finish(s, d, off, width, rows):
        origin = lax.rem(pos[RING[s]] + 4 - d, 4)
        cols = pl.ds(pl.multiple_of(s * HALF + origin * CH + off, 128), width)
        out_ref[:, cols] = 0.9 * mom_v[:, cols] + scale * rows.astype(jnp.float32)

    for s in BOTH:
        finish(s, 0, 0, CH, panel[s, pl.ds(0, ROWS), :])
    for b in every:
        with scope(f"fin{b}"):
            final[b].wait_recv()
        for s in BOTH:
            for d in (1, 2, 3):
                finish(s, d, *BATCHES[b], dec_r[s, d - 1, :, lanes(b)])
    with scope("sendwait"):
        for group in groups:
            group.wait_send()


def local(features, projection, out_grad, momentum):
    dma = pltpu.SemaphoreType.DMA
    f32, bf16 = jnp.float32, jnp.bfloat16
    return pl.pallas_call(
        kernel,
        out_shape=jax.ShapeDtypeStruct((ROWS, 2 * HALF), f32),
        in_specs=[pl.BlockSpec(memory_space=pltpu.HBM)] * 4,
        out_specs=pl.BlockSpec(memory_space=pltpu.VMEM),
        scratch_shapes=[
            pltpu.VMEM((TOK, KF), bf16),
            pltpu.VMEM((KF, R), bf16),
            pltpu.VMEM((2, 4 * TOK, CH), bf16),
            pltpu.VMEM((ROWS, 2 * HALF), f32),
            pltpu.VMEM((2, 4 * ROWS, R), bf16),
            pltpu.VMEM((TOK, R), f32),
            pltpu.VMEM((2, 128, R), f32),
            pltpu.VMEM((128, R), f32),
            pltpu.VMEM((2, R, 4 * TOK), bf16),
            pltpu.VMEM((2, R, CH), f32),
            pltpu.VMEM((2, R, CH), C_TYPE),
            pltpu.VMEM((2, 3, 64, CH), C_TYPE),
            pltpu.VMEM((2, 64, CH), f32),
            pltpu.VMEM((2, 3, 16, CH), f32),
            pltpu.VMEM((2, R, CH), E_TYPE),
            pltpu.VMEM((2, 3, ROWS, CH), G_TYPE),
            pltpu.VMEM((2, 3, ROWS, CH), G_TYPE),
            pltpu.VMEM((5, 8, 8, 128), f32),
            dma((13,)),
            dma((SEMS,)),
            dma((SEMS,)),
        ],
        compiler_params=pltpu.CompilerParams(
            collective_id=0, has_side_effects=True, vmem_limit_bytes=40 * 1024 * 1024,
        ),
        name="flora",
    )(*[pltpu.with_memory_space_constraint(a, pltpu.HBM) for a in (features, projection, out_grad, momentum)])


def solution(mesh):
    finer = Mesh(mesh.devices.reshape(4, 4, 4, 2, 2), ("zl", "x", "y", "zh", "c"))
    return jax.shard_map(
        local,
        mesh=finer,
        in_specs=(P(DP, MP), P(), P(DP, MP), P(DP, MP)),
        out_specs=P(DP, MP),
        check_vma=False,
    )
```

```python
import math

import jax
import jax.numpy as jnp
from jax import lax
from jax.experimental import pallas as pl
from jax.experimental.pallas import tpu as pltpu
from jax.sharding import Mesh
from jax.sharding import PartitionSpec as P

MESH = pl.DeviceIdType.MESH
FF = 20480
R = 256
TOK = 256
KF = 1792
ROWS = 112
COLS = 5120
CHUNK = (640, 512, 128)
BASE = (0, 2560, 4608)
RING = ("a", "b", "z")
CROSS = ("b", "a", "a")
THIRD = ("z", "z", "b")
BATCHES = (((0, 0, 384), (1, 0, 256)), ((0, 384, 256), (1, 256, 256)), ((2, 0, 128),))
Z = 2
LANES = sum(CHUNK)
C_TYPE = jnp.bfloat16
E_TYPE = jnp.bfloat16
G_TYPE = jnp.bfloat16
AHEAD = 3
SEMS = 16 + 6 * len(BATCHES)

MP = ("zh", "c")
DP = ("zl", "x", "y")
BOTH = (0, 1)


def segments():
    out, lane = [], 0
    for batch in BATCHES:
        out.append([])
        for s, off, width in batch:
            out[-1].append((s, off, width, pl.ds(lane, width)))
            lane += width
    return out


def dot(a, b):
    return jnp.dot(a, b, preferred_element_type=jnp.float32)


def tile_squares(v):
    rows, cols = v.shape
    total = jnp.zeros((8, 128), jnp.float32)
    for i in range(rows // 8):
        for j in range(cols // 128):
            part = v[8 * i : 8 * i + 8, 128 * j : 128 * j + 128]
            total = total + part * part
    return total


def kernel(
    f_hbm, p_hbm, g_hbm, m_hbm, out_ref,
    f_v, p_v, g_v, mom_v, pd_v,
    mpart, mrecv, msum, mixed,
    panel, panel_s, crecv, quart, drecv, full,
    dec_s, dec_r, sq,
    load_sem, ss, rs, ready,
):
    scope = jax.named_scope
    at = {a: lax.axis_index(a) for a in ("zl", "x", "y", "zh", "c")}
    zl, x, y, zh, c = (at[a] for a in ("zl", "x", "y", "zh", "c"))
    core, partner = {"c": 1 - c}, {"zh": 1 - zh}
    pos = {"a": x * (1 - c) + y * c, "b": x * c + y * (1 - c), "z": zl}
    groups = []
    segs = segments()
    every = range(len(BATCHES))

    def aligned(i, n):
        return pl.multiple_of(i * n, n)

    half, odd = lax.div(zl, 2), lax.rem(zl, 2)
    z_to = (3 - 3 * half, 2 - half, zl + 1 - 2 * odd)
    z_from = (2 - 2 * half, 3 - 2 * half, zl + 1 - 2 * odd)

    def step(axis, d):
        on_x = 1 - c if axis == "a" else c
        return {"x": lax.rem(x + d * on_x, 4), "y": lax.rem(y + d * (1 - on_x), 4)}

    peers = {axis: [(lax.rem(pos[axis] + d, 4), step(axis, d), d - 1) for d in (2, 1, 3)] for axis in ("a", "b")}
    peers["z"] = [(to, {"zl": to}, odd if j < 2 else 2) for j, to in enumerate(z_to)]

    def origin(axis, slot):
        return z_from[slot] if axis == "z" else lax.rem(pos[axis] + 3 - slot, 4)

    def remote(src, dst, i, where):
        return pltpu.make_async_remote_copy(
            src_ref=src, dst_ref=dst, send_sem=ss.at[i], recv_sem=rs.at[i],
            device_id=where, device_id_type=MESH,
        )

    def group_of(whole):
        groups.append(remote(whole, whole, len(groups), core))
        return len(groups) - 1

    def start(group, copies):
        for src, dst, where in copies:
            remote(src, dst, group, where).start()

    def send(copies, whole):
        group = group_of(whole)
        start(group, copies)
        return group

    def arrive(name, group):
        with scope(name):
            groups[group].wait_recv()

    def lanes(b):
        first = segs[b][0][3].start
        return pl.ds(first, sum(width for _, _, width, _ in segs[b]))

    barrier = pltpu.get_barrier_semaphore()
    greeted = [{axis: lax.rem(at[axis] + d, 4)} for axis in ("x", "y") for d in (1, 2, 3)] + [core]
    for where in greeted:
        pl.semaphore_signal(barrier, inc=1, device_id=where, device_id_type=MESH)

    def z_signal(sem, test, where):
        @pl.when(test)
        def _():
            pl.semaphore_signal(sem, inc=1, device_id=where, device_id_type=MESH)

    line = [lax.rem(zl + d, 4) for d in (1, 2, 3)]
    for z in line:
        z_signal(barrier, z > zl, {"zl": z})
    z_signal(barrier, zh == 0, partner)

    loads = {}

    def load(name, src, dst):
        copy = pltpu.make_async_copy(src, dst, load_sem.at[len(loads)])
        copy.start()
        loads[name] = copy

    load("f", f_hbm, f_v)
    load("p", p_hbm.at[pl.ds(aligned(zh * 2 + c, KF), KF), :], p_v)

    def columns(s, member, off, width):
        return pl.ds(pl.multiple_of(BASE[s] + member * CHUNK[s] + off, 128), width)

    def late_loads():
        for b in every:
            for s, off, width, seg in segs[b]:
                load(("g", b, s), g_hbm.at[:, columns(s, pos[RING[s]], off, width)], g_v.at[pl.ds(0, TOK), seg])
        here = {"zl": zl, "x": x, "y": y}
        for s, axis in enumerate(RING):
            for j, where in enumerate([{}] + [p[1] for p in peers[axis]]):
                w = here | where
                row = w["zl"] * 16 + w["x"] * 4 + w["y"]
                load(("p", s, j), p_hbm.at[pl.ds(aligned(row, ROWS), ROWS), :], pd_v.at[s, pl.ds(j * ROWS, ROWS), :])
        load("m", m_hbm, mom_v)

    grads = [group_of(g_v.at[pl.ds(TOK, 3 * TOK), lanes(b)]) for b in every]

    def grad_start(b):
        copies = []
        for j in range(3):
            for s, off, width, seg in segs[b]:
                to, where, slot = peers[RING[s]][j]
                copies.append((
                    g_hbm.at[:, columns(s, to, off, width)],
                    g_v.at[pl.ds(aligned(1 + slot, TOK), TOK), seg], where,
                ))
        start(grads[b], copies)

    def sum_send(b):
        arrive(f"got{b}", grads[b])
        for s, off, width, seg in segs[b]:
            loads["g", b, s].wait()
            panel[:, seg] = dot(mixed[s], g_v[:, seg])
            if C_TYPE != jnp.float32:
                panel_s[:, seg] = panel[:, seg].astype(C_TYPE)
        source = panel if C_TYPE == jnp.float32 else panel_s
        copies = []
        for j in range(3):
            for s, off, width, seg in segs[b]:
                to, where, slot = peers[CROSS[s]][j]
                copies.append((source.at[pl.ds(aligned(to, 64), 64), seg], crecv.at[slot, :, seg], where))
        return send(copies, crecv.at[:, :, lanes(b)])

    def reduce_send(b, group):
        arrive(f"C{b}", group)
        for s, off, width, seg in segs[b]:
            total = panel[pl.ds(aligned(pos[CROSS[s]], 64), 64), seg]
            for k in range(3):
                total = total + crecv[k, :, seg].astype(jnp.float32)
            quart[:, seg] = total
        copies = []
        for j in range(3):
            for s, off, width, seg in segs[b]:
                to, where, slot = peers[THIRD[s]][j]
                copies.append((quart.at[pl.ds(aligned(to, 16), 16), seg], drecv.at[slot, :, seg], where))
        return send(copies, drecv.at[:, :, lanes(b)])

    squares = []

    def gather_send(b, group):
        arrive(f"D{b}", group)
        places = {}
        for s, off, width, seg in segs[b]:
            total = quart[pl.ds(aligned(pos[THIRD[s]], 16), 16), seg]
            total = (total + drecv[2, :, seg]) + (drecv[0, :, seg] + drecv[1, :, seg])
            places[s] = pl.ds(pl.multiple_of(pos[CROSS[s]] * 64 + pos[THIRD[s]] * 16, 16), 16)
            full[places[s], seg] = total.astype(E_TYPE)
            squares.append(tile_squares(total))
        copies = []
        for j in range(3):
            for s, off, width, seg in segs[b]:
                piece = full.at[places[s], seg]
                copies.append((piece, piece, peers[THIRD[s]][j][1]))
        return send(copies, full.at[pl.ds(0, 48), lanes(b)])

    def cross_send(b, group):
        arrive(f"E{b}", group)
        copies = []
        for j in range(3):
            for s, off, width, seg in segs[b]:
                block = full.at[pl.ds(aligned(pos[CROSS[s]], 64), 64), seg]
                copies.append((block, block, peers[CROSS[s]][j][1]))
        return send(copies, full.at[pl.ds(0, 192), lanes(b)])

    def decode_send(b, group):
        arrive(f"F{b}", group)
        for s, off, width, seg in segs[b]:
            for j in range(4):
                if ("p", s, j) in loads:
                    loads.pop(("p", s, j)).wait()
            whole = full[:, seg]
            if E_TYPE == jnp.float32:
                high = whole.astype(jnp.bfloat16)
                low = (whole - high.astype(jnp.float32)).astype(jnp.bfloat16)
                rows = dot(pd_v[s], high) + dot(pd_v[s], low)
            else:
                rows = dot(pd_v[s], whole)
            panel[pl.ds(0, ROWS), seg] = rows[:ROWS]
            for j in range(3):
                dec_s[j, :, seg] = rows[(j + 1) * ROWS : (j + 2) * ROWS].astype(G_TYPE)
        copies = []
        for j in range(3):
            for s, off, width, seg in segs[b]:
                to, where, slot = peers[RING[s]][j]
                copies.append((dec_s.at[j, :, seg], dec_r.at[slot, :, seg], where))
        return send(copies, dec_r.at[:, :, lanes(b)])

    def spread(level, where):
        copies = [(sq.at[level, 0], sq.at[level, 1 + k], w) for k, w in enumerate(where)]
        return send(copies, sq.at[level, pl.ds(1, len(where))])

    def collect(level, group, n):
        arrive(f"sq{level}", group)
        total = sq[level, 0]
        for k in range(n):
            total = total + sq[level, 1 + k]
        sq[level + 1, 0] = total

    with scope("barrier"):
        pl.semaphore_wait(barrier, len(greeted) + zl + zh)
    grad_start(0)
    waits_long = zh * 4 + zl < AHEAD

    @pl.when(waits_long)
    def _():
        grad_start(1)

    for z in line:
        z_signal(ready.at[0], z < zl, {"zl": z})
    z_signal(ready.at[1], zh == 1, partner)
    mine = pl.ds(aligned(c, 128), 128)
    theirs = pl.ds(aligned(1 - c, 128), 128)
    with scope("mpart"):
        loads["f"].wait()
        loads["p"].wait()
        mpart[...] = dot(f_v[...], p_v[...])
    parts = [pl.ds(h * 128, 128) for h in BOTH]
    m1 = [send([(mpart.at[theirs, part], mrecv.at[0, :, part], core)], mrecv.at[0, :, part]) for part in parts]
    late_loads()
    m2 = []
    for h, part in enumerate(parts):
        arrive(f"m1{h}", m1[h])
        msum[:, part] = mpart[mine, part] + mrecv[0, :, part]
        if h == 0:

            @pl.when(zh == 0)
            def _():
                pl.semaphore_wait(ready.at[1], 1)

        m2.append(send([(msum.at[:, part], mrecv.at[1, :, part], partner)], msum.at[:, part]))

    @pl.when(zl < 3)
    def _():
        pl.semaphore_wait(ready.at[0], 3 - zl)


    def spot(s, part, slot):
        return mixed.at[s, part, pl.ds(pl.multiple_of((1 + slot) * TOK + c * 128, 128), 128)]

    direct, z_direct = {}, []
    passed = group_of(mixed.at[pl.ds(0, 2), :, pl.ds(0, 4 * 128)])
    z_passed = group_of(mixed.at[2, :, pl.ds(0, 4 * 128)])
    for h, part in enumerate(parts):
        arrive(f"m2{h}", m2[h])
        own = (msum[:, part] + mrecv[1, :, part]).T.astype(jnp.bfloat16)
        for s in range(3):
            mixed[s, part, mine] = own
        own = mixed.at[0, part, mine]
        for j in range(3):
            slot = peers["a"][j][2]
            direct[h, slot] = send(
                [(own, spot(s, part, slot), peers[RING[s]][j][1]) for s in BOTH],
                mixed.at[pl.ds(0, 2), part, pl.ds(0, 128)],
            )
        start(passed, [(mixed.at[s, part, mine], mixed.at[s, part, mine], core) for s in BOTH])
        start(z_passed, [(mixed.at[2, part, mine], mixed.at[2, part, mine], core)])
        z_direct.append(send(
            [(own, spot(2, part, slot), where) for _, where, slot in peers["z"]], mixed.at[2, part, pl.ds(0, 3 * 128)]
        ))

    grad_start(Z)

    @pl.when(jnp.logical_not(waits_long))
    def _():
        grad_start(1)

    for h, part in enumerate(parts):
        for slot in (0, 2, 1):
            arrive(f"direct{h}{slot}", direct[h, slot])
            start(passed, [(spot(s, part, slot), spot(1 - s, part, slot), core) for s in BOTH])
    arrive("passed", passed)
    moving = [sum_send(0), sum_send(1)]
    moving = [reduce_send(b, moving[b]) for b in BOTH]
    for h, part in enumerate(parts):
        arrive(f"z_direct{h}", z_direct[h])
        start(z_passed, [(spot(2, part, slot), spot(2, part, slot), core) for slot in range(3)])
    arrive("z_passed", z_passed)
    moving.append(sum_send(Z))
    moving[0] = gather_send(0, moving[0])
    moving[Z] = reduce_send(Z, moving[Z])
    moving[1] = gather_send(1, moving[1])
    moving[Z] = gather_send(Z, moving[Z])
    total = squares[0]
    for one in squares[1:]:
        total = total + one
    sq[0, 0] = total
    plane = [{"x": lax.rem(x + i, 4), "y": lax.rem(y + j, 4)} for i in range(4) for j in range(4) if i or j]
    q = spread(0, plane)
    moving = [cross_send(b, moving[b]) for b in every]
    collect(0, q, 15)
    stacked = [{"zl": z} for z in line] + [partner] + [{"zl": z} | partner for z in line]
    q = spread(1, [core] + [where | also for where in stacked for also in ({}, core)])
    final = {b: decode_send(b, moving[b]) for b in (0, Z, 1)}
    collect(1, q, 15)
    square_sum = jnp.sum(sq[2, 0], axis=(0, 1), keepdims=True)
    scale = 0.1 * (jnp.float32(math.sqrt(R * FF)) / jnp.sqrt(square_sum + 1e-06))

    loads["m"].wait()

    def finish(s, member, off, width, rows):
        cols = columns(s, member, off, width)
        out_ref[:, cols] = 0.9 * mom_v[:, cols] + scale * rows.astype(jnp.float32)

    for b in every:
        for s, off, width, seg in segs[b]:
            finish(s, pos[RING[s]], off, width, panel[pl.ds(0, ROWS), seg])
    for b in (0, Z, 1):
        arrive(f"fin{b}", final[b])
        for s, off, width, seg in segs[b]:
            for slot in range(3):
                finish(s, origin(RING[s], slot), off, width, dec_r[slot, :, seg])
    assert len(groups) == SEMS
    with scope("sendwait"):
        for group in groups:
            group.wait_send()


def local(features, projection, out_grad, momentum):
    dma = pltpu.SemaphoreType.DMA
    f32, bf16 = jnp.float32, jnp.bfloat16
    return pl.pallas_call(
        kernel,
        out_shape=jax.ShapeDtypeStruct((ROWS, COLS), f32),
        in_specs=[pl.BlockSpec(memory_space=pltpu.HBM)] * 4,
        out_specs=pl.BlockSpec(memory_space=pltpu.VMEM),
        scratch_shapes=[
            pltpu.VMEM((TOK, KF), bf16),
            pltpu.VMEM((KF, R), bf16),
            pltpu.VMEM((4 * TOK, LANES), bf16),
            pltpu.VMEM((ROWS, COLS), f32),
            pltpu.VMEM((3, 4 * ROWS, R), bf16),
            pltpu.VMEM((TOK, R), f32),
            pltpu.VMEM((2, 128, R), f32),
            pltpu.VMEM((128, R), f32),
            pltpu.VMEM((3, R, 4 * TOK), bf16),
            pltpu.VMEM((R, LANES), f32),
            pltpu.VMEM((R, LANES), C_TYPE),
            pltpu.VMEM((3, 64, LANES), C_TYPE),
            pltpu.VMEM((64, LANES), f32),
            pltpu.VMEM((3, 16, LANES), f32),
            pltpu.VMEM((R, LANES), E_TYPE),
            pltpu.VMEM((3, ROWS, LANES), G_TYPE),
            pltpu.VMEM((3, ROWS, LANES), G_TYPE),
            pltpu.VMEM((3, 16, 8, 128), f32),
            dma((20,)),
            dma((SEMS,)),
            dma((SEMS,)),
            pltpu.SemaphoreType.REGULAR((2,)),
        ],
        compiler_params=pltpu.CompilerParams(
            collective_id=0, has_side_effects=True, vmem_limit_bytes=40 * 1024 * 1024,
        ),
        name="flora",
    )(*[pltpu.with_memory_space_constraint(a, pltpu.HBM) for a in (features, projection, out_grad, momentum)])


def solution(mesh):
    finer = Mesh(mesh.devices.reshape(4, 4, 4, 2, 2), ("zl", "x", "y", "zh", "c"))
    return jax.shard_map(
        local,
        mesh=finer,
        in_specs=(P(DP, MP), P(), P(DP, MP), P(DP, MP)),
        out_specs=P(DP, MP),
        check_vma=False,
    )
```

```python
import math

import jax
import jax.numpy as jnp
from jax import lax
from jax.experimental import pallas as pl
from jax.experimental.pallas import tpu as pltpu
from jax.sharding import Mesh
from jax.sharding import PartitionSpec as P

MESH = pl.DeviceIdType.MESH
FF = 20480
R = 256
TOK = 256
KF = 1792
ROWS = 112
COLS = 5120
CHUNK = (640, 512, 128)
BASE = (0, 2560, 4608)
RING = ("a", "b", "z")
CROSS = ("b", "a", "a")
THIRD = ("z", "z", "b")
BATCHES = (((0, 0, 384), (1, 0, 256)), ((0, 384, 256), (1, 256, 256)), ((2, 0, 128),))
Z = 2
LANES = sum(CHUNK)
C_TYPE = jnp.bfloat16
E_TYPE = jnp.bfloat16
G_TYPE = jnp.bfloat16
AHEAD = 3
SEMS = 16 + 6 * len(BATCHES)

MP = ("zh", "c")
DP = ("zl", "x", "y")
BOTH = (0, 1)


def segments():
    out, lane = [], 0
    for batch in BATCHES:
        out.append([])
        for s, off, width in batch:
            out[-1].append((s, off, width, pl.ds(lane, width)))
            lane += width
    return out


def dot(a, b):
    return jnp.dot(a, b, preferred_element_type=jnp.float32)


def tile_squares(v):
    rows, cols = v.shape
    total = jnp.zeros((8, 128), jnp.float32)
    for i in range(rows // 8):
        for j in range(cols // 128):
            part = v[8 * i : 8 * i + 8, 128 * j : 128 * j + 128]
            total = total + part * part
    return total


def kernel(
    f_hbm, p_hbm, g_hbm, m_hbm, out_ref,
    f_v, p_v, g_v, mom_v, pd_v,
    mpart, mrecv, msum, mixed,
    panel, panel_s, crecv, quart, drecv, full,
    dec_s, dec_r, sq,
    load_sem, ss, rs, ready,
):
    scope = jax.named_scope
    at = {a: lax.axis_index(a) for a in ("zl", "x", "y", "zh", "c")}
    zl, x, y, zh, c = (at[a] for a in ("zl", "x", "y", "zh", "c"))
    core, partner = {"c": 1 - c}, {"zh": 1 - zh}
    pos = {"a": x * (1 - c) + y * c, "b": x * c + y * (1 - c), "z": zl}
    groups = []
    segs = segments()
    every = range(len(BATCHES))

    def aligned(i, n):
        return pl.multiple_of(i * n, n)

    half, odd = lax.div(zl, 2), lax.rem(zl, 2)
    z_to = (3 - 3 * half, 2 - half, zl + 1 - 2 * odd)
    z_from = (2 - 2 * half, 3 - 2 * half, zl + 1 - 2 * odd)

    def step(axis, d):
        on_x = 1 - c if axis == "a" else c
        return {"x": lax.rem(x + d * on_x, 4), "y": lax.rem(y + d * (1 - on_x), 4)}

    peers = {axis: [(lax.rem(pos[axis] + d, 4), step(axis, d), d - 1) for d in (2, 1, 3)] for axis in ("a", "b")}
    peers["z"] = [(to, {"zl": to}, odd if j < 2 else 2) for j, to in enumerate(z_to)]

    def origin(axis, slot):
        return z_from[slot] if axis == "z" else lax.rem(pos[axis] + 3 - slot, 4)

    def remote(src, dst, i, where):
        return pltpu.make_async_remote_copy(
            src_ref=src, dst_ref=dst, send_sem=ss.at[i], recv_sem=rs.at[i],
            device_id=where, device_id_type=MESH,
        )

    def group_of(whole):
        groups.append(remote(whole, whole, len(groups), core))
        return len(groups) - 1

    def start(group, copies):
        for src, dst, where in copies:
            remote(src, dst, group, where).start()

    def send(copies, whole):
        group = group_of(whole)
        start(group, copies)
        return group

    def arrive(name, group):
        with scope(name):
            groups[group].wait_recv()

    def lanes(b):
        first = segs[b][0][3].start
        return pl.ds(first, sum(width for _, _, width, _ in segs[b]))

    barrier = pltpu.get_barrier_semaphore()
    greeted = [{axis: lax.rem(at[axis] + d, 4)} for axis in ("x", "y") for d in (1, 2, 3)] + [core]
    for where in greeted:
        pl.semaphore_signal(barrier, inc=1, device_id=where, device_id_type=MESH)

    def z_signal(sem, test, where):
        @pl.when(test)
        def _():
            pl.semaphore_signal(sem, inc=1, device_id=where, device_id_type=MESH)

    line = [lax.rem(zl + d, 4) for d in (1, 2, 3)]
    for z in line:
        z_signal(barrier, z > zl, {"zl": z})
    z_signal(barrier, zh == 0, partner)

    loads = {}

    def load(name, src, dst):
        copy = pltpu.make_async_copy(src, dst, load_sem.at[len(loads)])
        copy.start()
        loads[name] = copy

    load("f", f_hbm, f_v)
    load("p", p_hbm.at[pl.ds(aligned(zh * 2 + c, KF), KF), :], p_v)

    def columns(s, member, off, width):
        return pl.ds(pl.multiple_of(BASE[s] + member * CHUNK[s] + off, 128), width)

    def late_loads():
        for b in every:
            for s, off, width, seg in segs[b]:
                load(("g", b, s), g_hbm.at[:, columns(s, pos[RING[s]], off, width)], g_v.at[pl.ds(0, TOK), seg])
        here = {"zl": zl, "x": x, "y": y}
        for s, axis in enumerate(RING):
            for j, where in enumerate([{}] + [p[1] for p in peers[axis]]):
                w = here | where
                row = w["zl"] * 16 + w["x"] * 4 + w["y"]
                load(("p", s, j), p_hbm.at[pl.ds(aligned(row, ROWS), ROWS), :], pd_v.at[s, pl.ds(j * ROWS, ROWS), :])
        load("m", m_hbm, mom_v)

    grads = [group_of(g_v.at[pl.ds(TOK, 3 * TOK), lanes(b)]) for b in every]

    def grad_start(b):
        copies = []
        for j in range(3):
            for s, off, width, seg in segs[b]:
                to, where, slot = peers[RING[s]][j]
                copies.append((
                    g_hbm.at[:, columns(s, to, off, width)],
                    g_v.at[pl.ds(aligned(1 + slot, TOK), TOK), seg], where,
                ))
        start(grads[b], copies)

    def sum_send(b):
        arrive(f"got{b}", grads[b])
        for s, off, width, seg in segs[b]:
            loads["g", b, s].wait()
            panel[:, seg] = dot(mixed[s], g_v[:, seg])
            if C_TYPE != jnp.float32:
                panel_s[:, seg] = panel[:, seg].astype(C_TYPE)
        source = panel if C_TYPE == jnp.float32 else panel_s
        copies = []
        for j in range(3):
            for s, off, width, seg in segs[b]:
                to, where, slot = peers[CROSS[s]][j]
                copies.append((source.at[pl.ds(aligned(to, 64), 64), seg], crecv.at[slot, :, seg], where))
        return send(copies, crecv.at[:, :, lanes(b)])

    def reduce_send(b, group):
        arrive(f"C{b}", group)
        for s, off, width, seg in segs[b]:
            total = panel[pl.ds(aligned(pos[CROSS[s]], 64), 64), seg]
            for k in range(3):
                total = total + crecv[k, :, seg].astype(jnp.float32)
            quart[:, seg] = total
        copies = []
        for j in range(3):
            for s, off, width, seg in segs[b]:
                to, where, slot = peers[THIRD[s]][j]
                copies.append((quart.at[pl.ds(aligned(to, 16), 16), seg], drecv.at[slot, :, seg], where))
        return send(copies, drecv.at[:, :, lanes(b)])

    squares = []

    def gather_send(b, group):
        arrive(f"D{b}", group)
        places = {}
        for s, off, width, seg in segs[b]:
            total = quart[pl.ds(aligned(pos[THIRD[s]], 16), 16), seg]
            total = (total + drecv[2, :, seg]) + (drecv[0, :, seg] + drecv[1, :, seg])
            places[s] = pl.ds(pl.multiple_of(pos[CROSS[s]] * 64 + pos[THIRD[s]] * 16, 16), 16)
            full[places[s], seg] = total.astype(E_TYPE)
            squares.append(tile_squares(total))
        copies = []
        for j in range(3):
            for s, off, width, seg in segs[b]:
                piece = full.at[places[s], seg]
                copies.append((piece, piece, peers[THIRD[s]][j][1]))
        return send(copies, full.at[pl.ds(0, 48), lanes(b)])

    def cross_send(b, group):
        arrive(f"E{b}", group)
        copies = []
        for j in range(3):
            for s, off, width, seg in segs[b]:
                block = full.at[pl.ds(aligned(pos[CROSS[s]], 64), 64), seg]
                copies.append((block, block, peers[CROSS[s]][j][1]))
        return send(copies, full.at[pl.ds(0, 192), lanes(b)])

    def decode_send(b, group):
        arrive(f"F{b}", group)
        for s, off, width, seg in segs[b]:
            for j in range(4):
                if ("p", s, j) in loads:
                    loads.pop(("p", s, j)).wait()
            whole = full[:, seg]
            if E_TYPE == jnp.float32:
                high = whole.astype(jnp.bfloat16)
                low = (whole - high.astype(jnp.float32)).astype(jnp.bfloat16)
                rows = dot(pd_v[s], high) + dot(pd_v[s], low)
            else:
                rows = dot(pd_v[s], whole)
            panel[pl.ds(0, ROWS), seg] = rows[:ROWS]
            for j in range(3):
                dec_s[j, :, seg] = rows[(j + 1) * ROWS : (j + 2) * ROWS].astype(G_TYPE)
        copies = []
        for j in range(3):
            for s, off, width, seg in segs[b]:
                to, where, slot = peers[RING[s]][j]
                copies.append((dec_s.at[j, :, seg], dec_r.at[slot, :, seg], where))
        return send(copies, dec_r.at[:, :, lanes(b)])

    def spread(level, where):
        copies = [(sq.at[level, 0], sq.at[level, 1 + k], w) for k, w in enumerate(where)]
        return send(copies, sq.at[level, pl.ds(1, len(where))])

    def collect(level, group, n):
        arrive(f"sq{level}", group)
        total = sq[level, 0]
        for k in range(n):
            total = total + sq[level, 1 + k]
        sq[level + 1, 0] = total

    with scope("mpart"):
        loads["f"].wait()
        loads["p"].wait()
        mpart[...] = dot(f_v[...], p_v[...])
    mine = pl.ds(aligned(c, 128), 128)
    theirs = pl.ds(aligned(1 - c, 128), 128)
    parts = [pl.ds(h * 128, 128) for h in BOTH]
    with scope("barrier"):
        pl.semaphore_wait(barrier, len(greeted) + zl + zh)
    m1 = [send([(mpart.at[theirs, part], mrecv.at[0, :, part], core)], mrecv.at[0, :, part]) for part in parts]
    grad_start(0)
    waits_long = zh * 4 + zl < AHEAD

    @pl.when(waits_long)
    def _():
        grad_start(1)

    for z in line:
        z_signal(ready.at[0], z < zl, {"zl": z})
    z_signal(ready.at[1], zh == 1, partner)
    late_loads()
    m2 = []
    for h, part in enumerate(parts):
        arrive(f"m1{h}", m1[h])
        msum[:, part] = mpart[mine, part] + mrecv[0, :, part]
        if h == 0:

            @pl.when(zh == 0)
            def _():
                pl.semaphore_wait(ready.at[1], 1)

        m2.append(send([(msum.at[:, part], mrecv.at[1, :, part], partner)], msum.at[:, part]))

    @pl.when(zl < 3)
    def _():
        pl.semaphore_wait(ready.at[0], 3 - zl)


    def spot(s, part, slot):
        return mixed.at[s, part, pl.ds(pl.multiple_of((1 + slot) * TOK + c * 128, 128), 128)]

    direct, z_direct = {}, []
    passed = group_of(mixed.at[pl.ds(0, 2), :, pl.ds(0, 4 * 128)])
    z_passed = group_of(mixed.at[2, :, pl.ds(0, 4 * 128)])
    for h, part in enumerate(parts):
        arrive(f"m2{h}", m2[h])
        own = (msum[:, part] + mrecv[1, :, part]).T.astype(jnp.bfloat16)
        for s in range(3):
            mixed[s, part, mine] = own
        own = mixed.at[0, part, mine]
        for j in range(3):
            slot = peers["a"][j][2]
            direct[h, slot] = send(
                [(own, spot(s, part, slot), peers[RING[s]][j][1]) for s in BOTH],
                mixed.at[pl.ds(0, 2), part, pl.ds(0, 128)],
            )
        start(passed, [(mixed.at[s, part, mine], mixed.at[s, part, mine], core) for s in BOTH])
        start(z_passed, [(mixed.at[2, part, mine], mixed.at[2, part, mine], core)])
        z_direct.append(send(
            [(own, spot(2, part, slot), where) for _, where, slot in peers["z"]], mixed.at[2, part, pl.ds(0, 3 * 128)]
        ))

    grad_start(Z)

    @pl.when(jnp.logical_not(waits_long))
    def _():
        grad_start(1)

    for h, part in enumerate(parts):
        for slot in (0, 2, 1):
            arrive(f"direct{h}{slot}", direct[h, slot])
            start(passed, [(spot(s, part, slot), spot(1 - s, part, slot), core) for s in BOTH])
    arrive("passed", passed)
    moving = [sum_send(0), sum_send(1)]
    moving = [reduce_send(b, moving[b]) for b in BOTH]
    for h, part in enumerate(parts):
        arrive(f"z_direct{h}", z_direct[h])
        start(z_passed, [(spot(2, part, slot), spot(2, part, slot), core) for slot in range(3)])
    arrive("z_passed", z_passed)
    moving.append(sum_send(Z))
    moving[0] = gather_send(0, moving[0])
    moving[Z] = reduce_send(Z, moving[Z])
    moving[1] = gather_send(1, moving[1])
    moving[Z] = gather_send(Z, moving[Z])
    total = squares[0]
    for one in squares[1:]:
        total = total + one
    sq[0, 0] = jnp.sum(total, axis=0, keepdims=True)
    plane = [{"x": lax.rem(x + i, 4), "y": lax.rem(y + j, 4)} for i in range(4) for j in range(4) if i or j]
    q = spread(0, plane)
    moving = [cross_send(b, moving[b]) for b in every]
    collect(0, q, 15)
    stacked = [{"zl": z} for z in line] + [partner] + [{"zl": z} | partner for z in line]
    q = spread(1, [core] + [where | also for where in stacked for also in ({}, core)])
    final = {b: decode_send(b, moving[b]) for b in every}
    collect(1, q, 15)
    square_sum = jnp.sum(sq[2, 0], axis=(0, 1), keepdims=True)
    scale = 0.1 * (jnp.float32(math.sqrt(R * FF)) / jnp.sqrt(square_sum + 1e-06))

    loads["m"].wait()

    def finish(s, member, off, width, rows):
        cols = columns(s, member, off, width)
        out_ref[:, cols] = 0.9 * mom_v[:, cols] + scale * rows.astype(jnp.float32)

    for b in every:
        for s, off, width, seg in segs[b]:
            finish(s, pos[RING[s]], off, width, panel[pl.ds(0, ROWS), seg])
    for b in every:
        arrive(f"fin{b}", final[b])
        for s, off, width, seg in segs[b]:
            for slot in range(3):
                finish(s, origin(RING[s], slot), off, width, dec_r[slot, :, seg])
    assert len(groups) == SEMS
    with scope("sendwait"):
        for group in groups:
            group.wait_send()


def local(features, projection, out_grad, momentum):
    dma = pltpu.SemaphoreType.DMA
    f32, bf16 = jnp.float32, jnp.bfloat16
    return pl.pallas_call(
        kernel,
        out_shape=jax.ShapeDtypeStruct((ROWS, COLS), f32),
        in_specs=[pl.BlockSpec(memory_space=pltpu.HBM)] * 4,
        out_specs=pl.BlockSpec(memory_space=pltpu.VMEM),
        scratch_shapes=[
            pltpu.VMEM((TOK, KF), bf16),
            pltpu.VMEM((KF, R), bf16),
            pltpu.VMEM((4 * TOK, LANES), bf16),
            pltpu.VMEM((ROWS, COLS), f32),
            pltpu.VMEM((3, 4 * ROWS, R), bf16),
            pltpu.VMEM((TOK, R), f32),
            pltpu.VMEM((2, 128, R), f32),
            pltpu.VMEM((128, R), f32),
            pltpu.VMEM((3, R, 4 * TOK), bf16),
            pltpu.VMEM((R, LANES), f32),
            pltpu.VMEM((R, LANES), C_TYPE),
            pltpu.VMEM((3, 64, LANES), C_TYPE),
            pltpu.VMEM((64, LANES), f32),
            pltpu.VMEM((3, 16, LANES), f32),
            pltpu.VMEM((R, LANES), E_TYPE),
            pltpu.VMEM((3, ROWS, LANES), G_TYPE),
            pltpu.VMEM((3, ROWS, LANES), G_TYPE),
            pltpu.VMEM((3, 16, 1, 128), f32),
            dma((20,)),
            dma((SEMS,)),
            dma((SEMS,)),
            pltpu.SemaphoreType.REGULAR((2,)),
        ],
        compiler_params=pltpu.CompilerParams(
            collective_id=0, has_side_effects=True, vmem_limit_bytes=40 * 1024 * 1024,
        ),
        name="flora",
    )(*[pltpu.with_memory_space_constraint(a, pltpu.HBM) for a in (features, projection, out_grad, momentum)])


def solution(mesh):
    finer = Mesh(mesh.devices.reshape(4, 4, 4, 2, 2), ("zl", "x", "y", "zh", "c"))
    return jax.shard_map(
        local,
        mesh=finer,
        in_specs=(P(DP, MP), P(), P(DP, MP), P(DP, MP)),
        out_specs=P(DP, MP),
        check_vma=False,
    )
```

```python
import math

import jax
import jax.numpy as jnp
from jax import lax
from jax.experimental import pallas as pl
from jax.experimental.pallas import tpu as pltpu
from jax.sharding import Mesh
from jax.sharding import PartitionSpec as P

MESH = pl.DeviceIdType.MESH
FF = 20480
R = 256
TOK = 256
KF = 1792
ROWS = 112
COLS = 5120
CHUNK = (640, 512, 128)
BASE = (0, 2560, 4608)
RING = ("a", "b", "z")
CROSS = ("b", "a", "a")
THIRD = ("z", "z", "b")
BATCHES = (((0, 0, 384), (1, 0, 256)), ((0, 384, 256), (1, 256, 256)), ((2, 0, 128),))
Z = 2
LANES = sum(CHUNK)
C_TYPE = jnp.bfloat16
E_TYPE = jnp.bfloat16
G_TYPE = jnp.bfloat16
AHEAD = 3
SEMS = 16 + 6 * len(BATCHES)

MP = ("zh", "c")
DP = ("zl", "x", "y")
BOTH = (0, 1)


def segments():
    out, lane = [], 0
    for batch in BATCHES:
        out.append([])
        for s, off, width in batch:
            out[-1].append((s, off, width, pl.ds(lane, width)))
            lane += width
    return out


def dot(a, b):
    return jnp.dot(a, b, preferred_element_type=jnp.float32)


def tile_squares(v):
    rows, cols = v.shape
    total = jnp.zeros((8, 128), jnp.float32)
    for i in range(rows // 8):
        for j in range(cols // 128):
            part = v[8 * i : 8 * i + 8, 128 * j : 128 * j + 128]
            total = total + part * part
    return total


def kernel(
    f_hbm, p_hbm, g_hbm, m_hbm, out_ref,
    f_v, p_v, g_v, mom_v, pd_v,
    mpart, mrecv, msum, mixed,
    panel, panel_s, crecv, quart, drecv, full,
    dec_s, dec_r, sq,
    load_sem, ss, rs, ready,
):
    scope = jax.named_scope
    at = {a: lax.axis_index(a) for a in ("zl", "x", "y", "zh", "c")}
    zl, x, y, zh, c = (at[a] for a in ("zl", "x", "y", "zh", "c"))
    core, partner = {"c": 1 - c}, {"zh": 1 - zh}
    pos = {"a": x * (1 - c) + y * c, "b": x * c + y * (1 - c), "z": zl}
    groups = []
    segs = segments()
    every = range(len(BATCHES))

    def aligned(i, n):
        return pl.multiple_of(i * n, n)

    half, odd = lax.div(zl, 2), lax.rem(zl, 2)
    z_to = (3 - 3 * half, 2 - half, zl + 1 - 2 * odd)
    z_from = (2 - 2 * half, 3 - 2 * half, zl + 1 - 2 * odd)

    def step(axis, d):
        on_x = 1 - c if axis == "a" else c
        return {"x": lax.rem(x + d * on_x, 4), "y": lax.rem(y + d * (1 - on_x), 4)}

    peers = {axis: [(lax.rem(pos[axis] + d, 4), step(axis, d), d - 1) for d in (2, 1, 3)] for axis in ("a", "b")}
    peers["z"] = [(to, {"zl": to}, odd if j < 2 else 2) for j, to in enumerate(z_to)]

    def origin(axis, slot):
        return z_from[slot] if axis == "z" else lax.rem(pos[axis] + 3 - slot, 4)

    def remote(src, dst, i, where):
        return pltpu.make_async_remote_copy(
            src_ref=src, dst_ref=dst, send_sem=ss.at[i], recv_sem=rs.at[i],
            device_id=where, device_id_type=MESH,
        )

    def group_of(whole):
        groups.append(remote(whole, whole, len(groups), core))
        return len(groups) - 1

    def start(group, copies):
        for src, dst, where in copies:
            remote(src, dst, group, where).start()

    def send(copies, whole):
        group = group_of(whole)
        start(group, copies)
        return group

    def arrive(name, group):
        with scope(name):
            groups[group].wait_recv()

    def lanes(b):
        first = segs[b][0][3].start
        return pl.ds(first, sum(width for _, _, width, _ in segs[b]))

    barrier = pltpu.get_barrier_semaphore()
    greeted = [{axis: lax.rem(at[axis] + d, 4)} for axis in ("x", "y") for d in (1, 2, 3)] + [core]
    for where in greeted:
        pl.semaphore_signal(barrier, inc=1, device_id=where, device_id_type=MESH)

    def z_signal(sem, test, where):
        @pl.when(test)
        def _():
            pl.semaphore_signal(sem, inc=1, device_id=where, device_id_type=MESH)

    line = [lax.rem(zl + d, 4) for d in (1, 2, 3)]
    for z in line:
        z_signal(barrier, z > zl, {"zl": z})
    z_signal(barrier, zh == 0, partner)

    loads = {}

    def load(name, src, dst):
        copy = pltpu.make_async_copy(src, dst, load_sem.at[len(loads)])
        copy.start()
        loads[name] = copy

    load("f", f_hbm, f_v)
    load("p", p_hbm.at[pl.ds(aligned(zh * 2 + c, KF), KF), :], p_v)

    def columns(s, member, off, width):
        return pl.ds(pl.multiple_of(BASE[s] + member * CHUNK[s] + off, 128), width)

    def late_loads():
        for b in every:
            for s, off, width, seg in segs[b]:
                load(("g", b, s), g_hbm.at[:, columns(s, pos[RING[s]], off, width)], g_v.at[pl.ds(0, TOK), seg])
        here = {"zl": zl, "x": x, "y": y}
        for s, axis in enumerate(RING):
            for j, where in enumerate([{}] + [p[1] for p in peers[axis]]):
                w = here | where
                row = w["zl"] * 16 + w["x"] * 4 + w["y"]
                load(("p", s, j), p_hbm.at[pl.ds(aligned(row, ROWS), ROWS), :], pd_v.at[s, pl.ds(j * ROWS, ROWS), :])
        load("m", m_hbm, mom_v)

    grads = [group_of(g_v.at[pl.ds(TOK, 3 * TOK), lanes(b)]) for b in every]

    def grad_start(b):
        copies = []
        for j in range(3):
            for s, off, width, seg in segs[b]:
                to, where, slot = peers[RING[s]][j]
                copies.append((
                    g_hbm.at[:, columns(s, to, off, width)],
                    g_v.at[pl.ds(aligned(1 + slot, TOK), TOK), seg], where,
                ))
        start(grads[b], copies)

    def sum_send(b):
        arrive(f"got{b}", grads[b])
        group = group_of(crecv.at[:, :, lanes(b)])
        for s, off, width, seg in segs[b]:
            loads["g", b, s].wait()
            panel[:, seg] = dot(mixed[s], g_v[:, seg])
            if C_TYPE != jnp.float32:
                panel_s[:, seg] = panel[:, seg].astype(C_TYPE)
            source = panel if C_TYPE == jnp.float32 else panel_s
            start(group, [
                (source.at[pl.ds(aligned(to, 64), 64), seg], crecv.at[slot, :, seg], where)
                for to, where, slot in peers[CROSS[s]]
            ])
        return group

    def reduce_send(b, group):
        arrive(f"C{b}", group)
        for s, off, width, seg in segs[b]:
            total = panel[pl.ds(aligned(pos[CROSS[s]], 64), 64), seg]
            for k in range(3):
                total = total + crecv[k, :, seg].astype(jnp.float32)
            quart[:, seg] = total
        copies = []
        for j in range(3):
            for s, off, width, seg in segs[b]:
                to, where, slot = peers[THIRD[s]][j]
                copies.append((quart.at[pl.ds(aligned(to, 16), 16), seg], drecv.at[slot, :, seg], where))
        return send(copies, drecv.at[:, :, lanes(b)])

    squares = []

    def gather_send(b, group):
        arrive(f"D{b}", group)
        places = {}
        for s, off, width, seg in segs[b]:
            total = quart[pl.ds(aligned(pos[THIRD[s]], 16), 16), seg]
            total = (total + drecv[2, :, seg]) + (drecv[0, :, seg] + drecv[1, :, seg])
            places[s] = pl.ds(pl.multiple_of(pos[CROSS[s]] * 64 + pos[THIRD[s]] * 16, 16), 16)
            full[places[s], seg] = total.astype(E_TYPE)
            squares.append(tile_squares(total))
        copies = []
        for j in range(3):
            for s, off, width, seg in segs[b]:
                piece = full.at[places[s], seg]
                copies.append((piece, piece, peers[THIRD[s]][j][1]))
        return send(copies, full.at[pl.ds(0, 48), lanes(b)])

    def cross_send(b, group):
        arrive(f"E{b}", group)
        copies = []
        for j in range(3):
            for s, off, width, seg in segs[b]:
                block = full.at[pl.ds(aligned(pos[CROSS[s]], 64), 64), seg]
                copies.append((block, block, peers[CROSS[s]][j][1]))
        return send(copies, full.at[pl.ds(0, 192), lanes(b)])

    def decode_send(b, group):
        arrive(f"F{b}", group)
        out = group_of(dec_r.at[:, :, lanes(b)])
        for s, off, width, seg in segs[b]:
            for j in range(4):
                if ("p", s, j) in loads:
                    loads.pop(("p", s, j)).wait()
            whole = full[:, seg]
            if E_TYPE == jnp.float32:
                high = whole.astype(jnp.bfloat16)
                low = (whole - high.astype(jnp.float32)).astype(jnp.bfloat16)
                rows = dot(pd_v[s], high) + dot(pd_v[s], low)
            else:
                rows = dot(pd_v[s], whole)
            panel[pl.ds(0, ROWS), seg] = rows[:ROWS]
            for j in range(3):
                dec_s[j, :, seg] = rows[(j + 1) * ROWS : (j + 2) * ROWS].astype(G_TYPE)
            start(out, [
                (dec_s.at[j, :, seg], dec_r.at[slot, :, seg], where)
                for j, (_, where, slot) in enumerate(peers[RING[s]])
            ])
        return out

    def spread(level, where):
        copies = [(sq.at[level, 0], sq.at[level, 1 + k], w) for k, w in enumerate(where)]
        return send(copies, sq.at[level, pl.ds(1, len(where))])

    def collect(level, group, n):
        arrive(f"sq{level}", group)
        total = sq[level, 0]
        for k in range(n):
            total = total + sq[level, 1 + k]
        sq[level + 1, 0] = total

    with scope("mpart"):
        loads["f"].wait()
        loads["p"].wait()
        mpart[...] = dot(f_v[...], p_v[...])
    mine = pl.ds(aligned(c, 128), 128)
    theirs = pl.ds(aligned(1 - c, 128), 128)
    parts = [pl.ds(h * 128, 128) for h in BOTH]
    with scope("barrier"):
        pl.semaphore_wait(barrier, len(greeted) + zl + zh)
    m1 = [send([(mpart.at[theirs, part], mrecv.at[0, :, part], core)], mrecv.at[0, :, part]) for part in parts]
    grad_start(0)
    waits_long = zh * 4 + zl < AHEAD

    @pl.when(waits_long)
    def _():
        grad_start(1)

    for z in line:
        z_signal(ready.at[0], z < zl, {"zl": z})
    z_signal(ready.at[1], zh == 1, partner)
    late_loads()
    m2 = []
    for h, part in enumerate(parts):
        arrive(f"m1{h}", m1[h])
        msum[:, part] = mpart[mine, part] + mrecv[0, :, part]
        if h == 0:

            @pl.when(zh == 0)
            def _():
                pl.semaphore_wait(ready.at[1], 1)

        m2.append(send([(msum.at[:, part], mrecv.at[1, :, part], partner)], msum.at[:, part]))

    @pl.when(zl < 3)
    def _():
        pl.semaphore_wait(ready.at[0], 3 - zl)


    def spot(s, part, slot):
        return mixed.at[s, part, pl.ds(pl.multiple_of((1 + slot) * TOK + c * 128, 128), 128)]

    direct, z_direct = {}, []
    passed = group_of(mixed.at[pl.ds(0, 2), :, pl.ds(0, 4 * 128)])
    z_passed = group_of(mixed.at[2, :, pl.ds(0, 4 * 128)])
    for h, part in enumerate(parts):
        arrive(f"m2{h}", m2[h])
        own = (msum[:, part] + mrecv[1, :, part]).T.astype(jnp.bfloat16)
        for s in range(3):
            mixed[s, part, mine] = own
        own = mixed.at[0, part, mine]
        for j in range(3):
            slot = peers["a"][j][2]
            direct[h, slot] = send(
                [(own, spot(s, part, slot), peers[RING[s]][j][1]) for s in BOTH],
                mixed.at[pl.ds(0, 2), part, pl.ds(0, 128)],
            )
        start(passed, [(mixed.at[s, part, mine], mixed.at[s, part, mine], core) for s in BOTH])
        start(z_passed, [(mixed.at[2, part, mine], mixed.at[2, part, mine], core)])
        z_direct.append(send(
            [(own, spot(2, part, slot), where) for _, where, slot in peers["z"]], mixed.at[2, part, pl.ds(0, 3 * 128)]
        ))

    grad_start(Z)

    @pl.when(jnp.logical_not(waits_long))
    def _():
        grad_start(1)

    for h, part in enumerate(parts):
        for slot in (0, 2, 1):
            arrive(f"direct{h}{slot}", direct[h, slot])
            start(passed, [(spot(s, part, slot), spot(1 - s, part, slot), core) for s in BOTH])
    arrive("passed", passed)
    moving = [sum_send(0), sum_send(1)]
    for h, part in enumerate(parts):
        arrive(f"z_direct{h}", z_direct[h])
        start(z_passed, [(spot(2, part, slot), spot(2, part, slot), core) for slot in range(3)])
    moving = [reduce_send(b, moving[b]) for b in BOTH]
    arrive("z_passed", z_passed)
    moving.append(sum_send(Z))
    moving[0] = gather_send(0, moving[0])
    moving[Z] = reduce_send(Z, moving[Z])
    moving[1] = gather_send(1, moving[1])
    moving[Z] = gather_send(Z, moving[Z])
    total = squares[0]
    for one in squares[1:]:
        total = total + one
    sq[0, 0] = jnp.sum(total, axis=0, keepdims=True)
    plane = [{"x": lax.rem(x + i, 4), "y": lax.rem(y + j, 4)} for i in range(4) for j in range(4) if i or j]
    q = spread(0, plane)
    moving = [cross_send(b, moving[b]) for b in every]
    collect(0, q, 15)
    stacked = [{"zl": z} for z in line] + [partner] + [{"zl": z} | partner for z in line]
    q = spread(1, [core] + [where | also for where in stacked for also in ({}, core)])
    final = {b: decode_send(b, moving[b]) for b in every}
    collect(1, q, 15)
    square_sum = jnp.sum(sq[2, 0], axis=(0, 1), keepdims=True)
    scale = 0.1 * (jnp.float32(math.sqrt(R * FF)) / jnp.sqrt(square_sum + 1e-06))

    loads["m"].wait()

    def finish(s, member, off, width, rows):
        cols = columns(s, member, off, width)
        out_ref[:, cols] = 0.9 * mom_v[:, cols] + scale * rows.astype(jnp.float32)

    for b in every:
        for s, off, width, seg in segs[b]:
            finish(s, pos[RING[s]], off, width, panel[pl.ds(0, ROWS), seg])
    for b in every:
        arrive(f"fin{b}", final[b])
        for s, off, width, seg in segs[b]:
            for slot in range(3):
                finish(s, origin(RING[s], slot), off, width, dec_r[slot, :, seg])
    assert len(groups) == SEMS
    with scope("sendwait"):
        for group in groups:
            group.wait_send()


def local(features, projection, out_grad, momentum):
    dma = pltpu.SemaphoreType.DMA
    f32, bf16 = jnp.float32, jnp.bfloat16
    return pl.pallas_call(
        kernel,
        out_shape=jax.ShapeDtypeStruct((ROWS, COLS), f32),
        in_specs=[pl.BlockSpec(memory_space=pltpu.HBM)] * 4,
        out_specs=pl.BlockSpec(memory_space=pltpu.VMEM),
        scratch_shapes=[
            pltpu.VMEM((TOK, KF), bf16),
            pltpu.VMEM((KF, R), bf16),
            pltpu.VMEM((4 * TOK, LANES), bf16),
            pltpu.VMEM((ROWS, COLS), f32),
            pltpu.VMEM((3, 4 * ROWS, R), bf16),
            pltpu.VMEM((TOK, R), f32),
            pltpu.VMEM((2, 128, R), f32),
            pltpu.VMEM((128, R), f32),
            pltpu.VMEM((3, R, 4 * TOK), bf16),
            pltpu.VMEM((R, LANES), f32),
            pltpu.VMEM((R, LANES), C_TYPE),
            pltpu.VMEM((3, 64, LANES), C_TYPE),
            pltpu.VMEM((64, LANES), f32),
            pltpu.VMEM((3, 16, LANES), f32),
            pltpu.VMEM((R, LANES), E_TYPE),
            pltpu.VMEM((3, ROWS, LANES), G_TYPE),
            pltpu.VMEM((3, ROWS, LANES), G_TYPE),
            pltpu.VMEM((3, 16, 1, 128), f32),
            dma((20,)),
            dma((SEMS,)),
            dma((SEMS,)),
            pltpu.SemaphoreType.REGULAR((2,)),
        ],
        compiler_params=pltpu.CompilerParams(
            collective_id=0, has_side_effects=True, vmem_limit_bytes=40 * 1024 * 1024,
        ),
        name="flora",
    )(*[pltpu.with_memory_space_constraint(a, pltpu.HBM) for a in (features, projection, out_grad, momentum)])


def solution(mesh):
    finer = Mesh(mesh.devices.reshape(4, 4, 4, 2, 2), ("zl", "x", "y", "zh", "c"))
    return jax.shard_map(
        local,
        mesh=finer,
        in_specs=(P(DP, MP), P(), P(DP, MP), P(DP, MP)),
        out_specs=P(DP, MP),
        check_vma=False,
    )
```
